32 devices in a mesh: gx: 4 (over x, core), gy: 8 (over z, y).
Axes of the slice: x: 2, y: 2, z: 4, core: 2. Of those that a mesh axis runs over, the one named last changes fastest.
Arguments:
- east_velocity: float32 [48, 32, 2048], P(None, 'gx', 'gy'), may hold values from -3 to 3
- north_velocity: float32 [48, 32, 2048], P(None, 'gx', 'gy'), may hold values from -3 to 3
- salinity: float32 [48, 32, 2048], P(None, 'gx', 'gy'), may hold values from -6 to 6
- surface: float32 [32, 2048], P('gx', 'gy'), may hold values from -6 to 6
- column_depth: float32 [32, 2048], P('gx', 'gy'), may hold values from 0.5 to 4
- wet_column: int32 [32, 2048], P('gx', 'gy'), may hold values 0 or 1
- active_levels: int32 [32, 2048], P('gx', 'gy'), may hold values from 1 to 48
Outputs:
- east_flow: float32 [48, 32, 2048], P(None, 'gx', 'gy')
- north_flow: float32 [48, 32, 2048], P(None, 'gx', 'gy')
- salt_next: float32 [48, 32, 2048], P(None, 'gx', 'gy')
- surface_next: float32 [32, 2048], P('gx', 'gy')
The draws below stay inside these ranges and needn't reach their ends.
All inputs are finite; a program needn't handle non-finite values. No bound on the sum of `wet_column` on one device may be relied on, other than what follows from the above.
Results may differ from the reference program's by a relative error of at most 0.000024.
Values sent between devices are 32-bit elements; how exact they have to be, the bound alone decides.
A program may use at most 64 MiB of HBM per device.

```python
import math
import jax
import jax.numpy as jnp

LEV = 48
ITERS = 16
NX = 32
NY = 2048


def touch_ends(values, key, least, largest):
    spot = [jax.random.randint(jax.random.fold_in(key, axis), (), 0, length) for axis, length in enumerate(values.shape)]
    main_axis = values.shape.index(max(values.shape))
    neighbour = spot[:main_axis] + [(spot[main_axis] + 1) % values.shape[main_axis]] + spot[main_axis + 1:]
    return values.at[tuple(spot)].set(least).at[tuple(neighbour)].set(largest)


def level_of(own_key, shape, shards, low, high):
    gain = 1.0
    for position, blocks in shards:
        steps = jax.random.uniform(jax.random.fold_in(jax.random.fold_in(own_key, 6), position), (blocks,), jnp.float32, low / len(shards), high / len(shards))
        gain = gain * jnp.repeat(jnp.exp(steps), shape[position] // blocks).reshape((-1,) + (1,) * (len(shape) - 1 - position))
    return gain


def normal_values(own_key, shape, scale, reach, pieces=(), held_as=jnp.bfloat16):
    entries = jax.random.normal(own_key, shape, jnp.float32) * scale
    if len(pieces) > 0:
        entries = level_of(own_key, shape, pieces, -0.22, 0.18) * entries
    return jnp.clip(entries, min=-reach, max=reach).astype(held_as)


def setup_inputs(seed: int = 0) -> dict:
    arg_keys = jax.random.split(jax.random.key(seed), 8)
    east_velocity = normal_values(arg_keys[0], (LEV, NX, NY), 0.5, 3.0, ((1, 4), (2, 8)), jnp.float32)
    north_velocity = normal_values(arg_keys[1], (LEV, NX, NY), 0.5, 3.0, ((1, 4), (2, 8)), jnp.float32)
    salinity = normal_values(arg_keys[2], (LEV, NX, NY), 1.0, 6.0, ((1, 4), (2, 8)), jnp.float32)
    surface = normal_values(arg_keys[3], (NX, NY), 1.0, 6.0, ((0, 4), (1, 8)), jnp.float32)
    column_depth = jnp.clip(jnp.exp(math.log(4.0) - 2.0794415 * jax.random.uniform(arg_keys[4], (NX, NY), jnp.float32) ** level_of(arg_keys[4], (NX, NY), ((0, 4), (1, 8)), -0.2, 0.2)), 0.5, 4.0)
    wet_column = touch_ends((jax.random.randint(arg_keys[5], (NX, NY), 0, 8) < 7).astype(jnp.int32), jax.random.fold_in(arg_keys[5], 1), 0, 1)
    active_levels = touch_ends(jax.random.randint(arg_keys[6], (NX, NY), 1, LEV + 1), jax.random.fold_in(arg_keys[6], 1), 1, LEV).astype(jnp.int32)
    return {"east_velocity": east_velocity, "north_velocity": north_velocity, "salinity": salinity, "surface": surface, "column_depth": column_depth, "wet_column": wet_column, "active_levels": active_levels}


TIME_STEP = 0.2
CORIOLIS = 0.3
PRESS_COEF = 0.05
VISCOSITY = 0.1
DIFFUSIVITY = 0.1
SIGMA_SHIFT = 0.25
CHEB_CENTER = 3.625
CHEB_HALF = 3.375
DIVERGENCE_COEF = 8.0


def cheb_table(count):
    first = CHEB_CENTER / CHEB_HALF
    ratio = 1.0 / first
    keeps = []
    gains = []
    for index in range(count):
        ratio_next = 1.0 / (2.0 * first - ratio)
        keeps.append(ratio_next * ratio)
        gains.append(2.0 * ratio_next / CHEB_HALF)
        ratio = ratio_next
    return keeps, gains


def centre(field):
    return field[:, 2:-2, 2:-2]


def along_east(field):
    return (8.0 * (field[:, 3:-1, 2:-2] - field[:, 1:-3, 2:-2]) - (field[:, 4:, 2:-2] - field[:, :-4, 2:-2])) / 12.0


def along_north(field):
    return (8.0 * (field[:, 2:-2, 3:-1] - field[:, 2:-2, 1:-3]) - (field[:, 2:-2, 4:] - field[:, 2:-2, :-4])) / 12.0


def laplace(field):
    return field[:, 3:-1, 2:-2] + field[:, 1:-3, 2:-2] + field[:, 2:-2, 3:-1] + field[:, 2:-2, 1:-3] - 4.0 * centre(field)


def tendency(padded):
    east, north, tracer = padded[0], padded[1], padded[2]
    pressure = PRESS_COEF * jnp.cumsum(tracer, axis=0)
    east_mid = centre(east)
    north_mid = centre(north)

    def advect(field):
        return -(east_mid * along_east(field) + north_mid * along_north(field))

    east_rate = advect(east) + CORIOLIS * north_mid - along_east(pressure) + VISCOSITY * laplace(east)
    north_rate = advect(north) - CORIOLIS * east_mid - along_north(pressure) + VISCOSITY * laplace(north)
    salt_rate = advect(tracer) + DIFFUSIVITY * laplace(tracer)
    return jnp.stack([east_rate, north_rate, salt_rate])


def nine_point(field, wet):
    weighted = wet * field
    edges = weighted[2:, 1:-1] + weighted[:-2, 1:-1] + weighted[1:-1, 2:] + weighted[1:-1, :-2]
    corners = weighted[2:, 2:] + weighted[2:, :-2] + weighted[:-2, 2:] + weighted[:-2, :-2]
    stencil = (20.0 * weighted[1:-1, 1:-1] - 4.0 * edges - corners) / 6.0
    wet_mid = wet[1:-1, 1:-1]
    field_mid = field[1:-1, 1:-1]
    return wet_mid * (SIGMA_SHIFT * field_mid + stencil) + (1.0 - wet_mid) * field_mid


def reference(east_velocity, north_velocity, salinity, surface, column_depth, wet_column, active_levels):
    wet = wet_column.astype(jnp.float32)
    levels = jnp.arange(LEV, dtype=jnp.int32)
    mask3 = (levels[:, None, None] < active_levels[None]).astype(jnp.float32) * wet[None]
    state0 = jnp.stack([east_velocity, north_velocity, salinity]) * mask3

    def rate(state):
        padded = jnp.pad(state, ((0, 0), (0, 0), (2, 2), (2, 2)))
        return tendency(padded) * mask3

    state1 = state0 + TIME_STEP * rate(state0)
    state2 = 0.75 * state0 + 0.25 * (state1 + TIME_STEP * rate(state1))
    state3 = state0 / 3.0 + (2.0 / 3.0) * (state2 + TIME_STEP * rate(state2))
    flow_east = column_depth * (jnp.sum(state3[0], axis=0) / LEV)
    flow_north = column_depth * (jnp.sum(state3[1], axis=0) / LEV)
    east_pad = jnp.pad(flow_east, 1)
    north_pad = jnp.pad(flow_north, 1)
    divergence = (east_pad[2:, 1:-1] - east_pad[:-2, 1:-1]) * 0.5 + (north_pad[1:-1, 2:] - north_pad[1:-1, :-2]) * 0.5
    right_side = wet * (SIGMA_SHIFT * surface - DIVERGENCE_COEF * divergence)
    wet_pad = jnp.pad(wet, 1)

    def apply(field):
        return nine_point(jnp.pad(field, 1), wet_pad)

    solution = surface
    residual = right_side - apply(solution)
    direction = residual / CHEB_CENTER
    keeps, gains = cheb_table(ITERS)
    for index in range(ITERS):
        solution = solution + direction
        residual = residual - apply(direction)
        direction = keeps[index] * direction + gains[index] * residual
    surface_pad = jnp.pad(solution, 1)
    slope_east = (surface_pad[2:, 1:-1] - surface_pad[:-2, 1:-1]) * 0.5
    slope_north = (surface_pad[1:-1, 2:] - surface_pad[1:-1, :-2]) * 0.5
    east_flow = mask3 * (state3[0] - slope_east[None])
    north_flow = mask3 * (state3[1] - slope_north[None])
    return east_flow, north_flow, state3[2], solution
```

```python
import functools

import jax
import jax.numpy as jnp
from jax import lax
from jax.experimental import pallas as pl
from jax.experimental.pallas import tpu as pltpu
from jax.sharding import PartitionSpec as P

ITERS = 16

TIME_STEP = 0.2
CORIOLIS = 0.3
PRESS_COEF = 0.05
VISCOSITY = 0.1
DIFFUSIVITY = 0.1
SIGMA_SHIFT = 0.25
CHEB_CENTER = 3.625
CHEB_HALF = 3.375
DIVERGENCE_COEF = 8.0

ROWS = 8
LANES = 128
CHUNK = 8
MESH = pl.DeviceIdType.MESH


def cheb_table(count):
    first = CHEB_CENTER / CHEB_HALF
    ratio = 1.0 / first
    keeps = []
    gains = []
    for index in range(count):
        ratio_next = 1.0 / (2.0 * first - ratio)
        keeps.append(ratio_next * ratio)
        gains.append(2.0 * ratio_next / CHEB_HALF)
        ratio = ratio_next
    return (keeps, gains)


def kernel(
    nx, ny, reach, slots,
    east_ref, north_ref, salt_ref, surface_ref, depth_ref, wet_ref, active_ref,
    east_out, north_out, salt_out, surface_out,
    q0, qa, qb, send_x, recv_x, send_y, recv_y,
    stat_c, stat_e, flow_c, flow_e, all_stat, rim_stat, all_flow, rim_flow, xs,
    x_send, x_recv, y_send, y_recv,
    stat_send, stat_recv, stat_rim_send, stat_rim_recv,
    flow_send, flow_recv, flow_rim_send, flow_rim_recv,
):
    gx = lax.axis_index("gx")
    gy = lax.axis_index("gy")
    levels = east_ref.shape[0]
    width = east_ref.shape[2]
    tiles = width // LANES
    chunks = levels // CHUNK
    groups = 3 * CHUNK // 4
    relative = slots < nx
    row = lax.broadcasted_iota(jnp.int32, (ROWS, LANES), 0)
    lane = lax.broadcasted_iota(jnp.int32, (ROWS, LANES), 1)
    pair = row // 2
    zero = jnp.zeros((ROWS, LANES), jnp.float32)

    def lanes(t):
        return slice(t * LANES, (t + 1) * LANES)

    def slot_in(owner, peer):
        return owner - peer + reach if relative else owner

    def inside(x, y):
        return jnp.logical_and(
            jnp.logical_and(x >= 0, x < nx), jnp.logical_and(y >= 0, y < ny)
        )

    offsets = [o for o in range(-reach, reach + 1)]
    partners = [(o, side) for o in offsets for side in (-1, 0, 1) if (o, side) != (0, 0)]

    barrier = pltpu.get_barrier_semaphore()
    count = jnp.int32(0)
    for o, side in partners:
        there = inside(gx + o, gy + side)

        @pl.when(there)
        def _(o=o, side=side):
            pl.semaphore_signal(
                barrier, inc=1, device_id=(gx + o, gy + side), device_id_type=MESH
            )

        count = count + there.astype(jnp.int32)

    own = slot_in(gx, gx)

    for side, missing in ((0, gx == 0), (1, gx == nx - 1)):
        @pl.when(missing)
        def _(side=side):
            for stage in range(3):
                @pl.loop(0, chunks)
                def _(c, stage=stage):
                    recv_x[stage, side, c] = jnp.zeros((groups, ROWS, width), jnp.float32)

    for side, missing in ((0, gy == 0), (1, gy == ny - 1)):
        @pl.when(missing)
        def _(side=side):
            recv_y[:, side] = jnp.zeros((3, chunks, ROWS, LANES), jnp.float32)
            rim_stat[side] = jnp.zeros((slots, 2, ROWS, LANES), jnp.float32)
            rim_flow[side] = jnp.zeros((slots, 2, ROWS, LANES), jnp.float32)

    if relative:
        for o in offsets:
            @pl.when(jnp.logical_not(inside(gx + o, gy)))
            def _(o=o):
                for block in (all_stat, all_flow):
                    block[o + reach] = jnp.zeros((2, ROWS, width), jnp.float32)
                for block in (rim_stat, rim_flow):
                    for side in range(2):
                        block[side, o + reach] = jnp.zeros((2, ROWS, LANES), jnp.float32)

    def pack(state, stage, c):
        rim = zero
        for f in range(3):
            for half in range(CHUNK // 4):
                group = f * (CHUNK // 4) + half
                ups = [None] * tiles
                downs = [None] * tiles
                for m in range(4):
                    k = c * CHUNK + half * 4 + m
                    position = group * 4 + m
                    parts = [state[f, k, :, lanes(t)] for t in range(tiles)]
                    for t in range(tiles):
                        turned = parts[t] if m == 3 else pltpu.roll(parts[t], 2 * m + 2, 0)
                        if m == 0:
                            ups[t] = turned
                            downs[t] = turned
                        else:
                            ups[t] = jnp.where(pair == m, turned, ups[t])
                            downs[t] = jnp.where(pair == (m + 1) % 4, turned, downs[t])
                    ends = jnp.where(lane < LANES // 2, parts[0], parts[-1])
                    rim = jnp.where(
                        lane // 4 == position,
                        pltpu.roll(ends, (4 * position + 2) % LANES, 1),
                        rim,
                    )
                for t in range(tiles):
                    send_x[stage, 0, c, group, :, lanes(t)] = downs[t]
                    send_x[stage, 1, c, group, :, lanes(t)] = ups[t]
        send_y[stage, c] = rim

    def x_copy(stage, c, side):
        return pltpu.make_async_remote_copy(
            src_ref=send_x.at[stage, side, c],
            dst_ref=recv_x.at[stage, 1 - side, c],
            send_sem=x_send.at[stage, side, c],
            recv_sem=x_recv.at[stage, 1 - side, c],
            device_id=(gx + 2 * side - 1, gy),
            device_id_type=MESH,
        )

    def y_copy(stage, c, side):
        return pltpu.make_async_remote_copy(
            src_ref=send_y.at[stage, c],
            dst_ref=recv_y.at[stage, 1 - side, c],
            send_sem=y_send.at[stage, side, c],
            recv_sem=y_recv.at[stage, 1 - side, c],
            device_id=(gx, gy + 2 * side - 1),
            device_id_type=MESH,
        )

    near = [
        (x_copy, 0, gx > 0), (x_copy, 1, gx < nx - 1),
        (y_copy, 0, gy > 0), (y_copy, 1, gy < ny - 1),
    ]

    def launch(stage, c):
        for copy, side, there in near:
            @pl.when(there)
            def _(copy=copy, side=side):
                copy(stage, c, side).start()

    def arrive(stage, c):
        for copy, side, there in near:
            @pl.when(there)
            def _(copy=copy, side=side):
                copy(stage, c, 1 - side).wait_recv()

    def drain(stage, c):
        for copy, side, there in near:
            @pl.when(there)
            def _(copy=copy, side=side):
                copy(stage, c, side).wait_send()

    def far_copy(kind, o, side):
        block, rim, everything, edge, ss, rs, rss, rrs = kind
        slot = slot_in(gx, gx + o)
        if side == 0:
            return pltpu.make_async_remote_copy(
                src_ref=block, dst_ref=everything.at[slot],
                send_sem=ss.at[o + reach], recv_sem=rs.at[slot],
                device_id=(gx + o, gy), device_id_type=MESH,
            )
        to = (1 - side) // 2
        return pltpu.make_async_remote_copy(
            src_ref=rim, dst_ref=edge.at[to, slot],
            send_sem=rss.at[to, o + reach], recv_sem=rrs.at[to, slot],
            device_id=(gx + o, gy + side), device_id_type=MESH,
        )

    def far_wait(kind, o, side):
        block, rim, everything, edge, ss, rs, rss, rrs = kind
        slot = slot_in(gx + o, gx)
        if side == 0:
            pltpu.make_async_remote_copy(
                src_ref=block, dst_ref=everything.at[slot],
                send_sem=ss.at[o + reach], recv_sem=rs.at[slot],
                device_id=(gx + o, gy), device_id_type=MESH,
            ).wait_recv()
        else:
            at = (1 + side) // 2
            pltpu.make_async_remote_copy(
                src_ref=rim, dst_ref=edge.at[at, slot],
                send_sem=rss.at[at, o + reach], recv_sem=rrs.at[at, slot],
                device_id=(gx + o, gy + side), device_id_type=MESH,
            ).wait_recv()

    def far(action):
        for o, side in partners:
            @pl.when(inside(gx + o, gy + side))
            def _(o=o, side=side):
                action(o, side)

    stat_kind = (stat_c, stat_e, all_stat, rim_stat,
                 stat_send, stat_recv, stat_rim_send, stat_rim_recv)
    flow_kind = (flow_c, flow_e, all_flow, rim_flow,
                 flow_send, flow_recv, flow_rim_send, flow_rim_recv)

    active = [active_ref[:, lanes(t)] * wet_ref[:, lanes(t)] for t in range(tiles)]
    inputs = (east_ref, north_ref, salt_ref)

    def mask_chunk(c):
        for kk in range(CHUNK):
            k = c * CHUNK + kk
            for t in range(tiles):
                live = active[t] > k
                for f in range(3):
                    q0[f, k, :, lanes(t)] = jnp.where(live, inputs[f][k, :, lanes(t)], 0.0)

    def first(c, carry):
        mask_chunk(c)
        pack(q0, 0, c)
        return carry

    lax.fori_loop(0, chunks, first, 0)

    stat_parts = (
        [surface_ref[:, lanes(t)] for t in range(tiles)],
        [wet_ref[:, lanes(t)].astype(jnp.float32) for t in range(tiles)],
    )
    for f in range(2):
        for t in range(tiles):
            stat_c[f, :, lanes(t)] = stat_parts[f][t]
            all_stat[own, f, :, lanes(t)] = stat_parts[f][t]
        stat_e[f] = jnp.where(lane < LANES // 2, stat_parts[f][0], stat_parts[f][-1])

    pl.semaphore_wait(barrier, count)

    def first_launch(c, carry):
        launch(0, c)
        return carry

    lax.fori_loop(0, chunks, first_launch, 0)
    far(lambda o, side: far_copy(stat_kind, o, side).start())

    def slope8(a, b, c, d):
        return 8.0 * (a - b) - (c - d)

    def run_stage(stage, src, dst, weight0, weight1):
        def body(c, carry):
            press_e, press_n, sum_e, sum_n = [list(x) for x in carry]
            arrive(stage, c)
            rims = jnp.where(lane % 4 < 2, recv_y[stage, 0, c], recv_y[stage, 1, c])
            for kk in range(CHUNK):
                k = c * CHUNK + kk
                fields = []
                for f in range(3):
                    position = f * CHUNK + kk
                    group, m = position // 4, position % 4
                    rim = pltpu.roll(rims, (-(4 * position + 2)) % LANES, 1)
                    parts = [src[f, k, :, lanes(t)] for t in range(tiles)]
                    per_tile = []
                    for t in range(tiles):
                        q = parts[t]
                        after = parts[t + 1] if t + 1 < tiles else rim
                        before = parts[t - 1] if t > 0 else rim
                        ends = jnp.where(
                            pair == m,
                            recv_x[stage, 0, c, group, :, lanes(t)],
                            recv_x[stage, 1, c, group, :, lanes(t)],
                        )
                        if m != 3:
                            ends = pltpu.roll(ends, (-(2 * m + 2)) % ROWS, 0)
                        e1 = pltpu.roll(jnp.where(row < 1, ends, q), ROWS - 1, 0)
                        e2 = pltpu.roll(jnp.where(row < 2, ends, q), ROWS - 2, 0)
                        w1 = pltpu.roll(jnp.where(row >= ROWS - 1, ends, q), 1, 0)
                        w2 = pltpu.roll(jnp.where(row >= ROWS - 2, ends, q), 2, 0)
                        n1 = pltpu.roll(jnp.where(lane < 1, after, q), LANES - 1, 1)
                        n2 = pltpu.roll(jnp.where(lane < 2, after, q), LANES - 2, 1)
                        s1 = pltpu.roll(jnp.where(lane >= LANES - 1, before, q), 1, 1)
                        s2 = pltpu.roll(jnp.where(lane >= LANES - 2, before, q), 2, 1)
                        dx = slope8(e1, w1, e2, w2)
                        dy = slope8(n1, s1, n2, s2)
                        lap = ((e1 + w1) + (n1 + s1)) - 4.0 * q
                        per_tile.append((q, dx, dy, lap))
                    fields.append(per_tile)
                for t in range(tiles):
                    live = active[t] > k
                    (u, ux, uy, ul), (v, vx, vy, vl), (s, sx, sy, sl) = [
                        fields[f][t] for f in range(3)
                    ]
                    press_e[t] = press_e[t] + sx
                    press_n[t] = press_n[t] + sy
                    um = u * (-1.0 / 12.0)
                    vm = v * (-1.0 / 12.0)
                    coef = -PRESS_COEF / 12.0
                    ru = (um * ux + vm * uy) + CORIOLIS * v + coef * press_e[t] + VISCOSITY * ul
                    rv = (um * vx + vm * vy) - CORIOLIS * u + coef * press_n[t] + VISCOSITY * vl
                    rs = (um * sx + vm * sy) + DIFFUSIVITY * sl
                    news = []
                    for f, (q, rate) in enumerate(((u, ru), (v, rv), (s, rs))):
                        new = q + TIME_STEP * rate
                        if weight0 is not None:
                            new = weight0 * q0[f, k, :, lanes(t)] + weight1 * new
                        new = jnp.where(live, new, 0.0)
                        news.append(new)
                        if stage == 2 and f == 2:
                            salt_out[k, :, lanes(t)] = new
                        else:
                            dst[f, k, :, lanes(t)] = new
                    if stage == 2:
                        sum_e[t] = sum_e[t] + news[0]
                        sum_n[t] = sum_n[t] + news[1]
            if stage < 2:
                pack(dst, stage + 1, c)
                launch(stage + 1, c)
            return (tuple(press_e), tuple(press_n), tuple(sum_e), tuple(sum_n))

        zeros = (zero,) * tiles
        return lax.fori_loop(0, chunks, body, (zeros, zeros, zeros, zeros))

    run_stage(0, q0, qa, None, None)
    run_stage(1, qa, qb, 0.75, 0.25)
    carry = run_stage(2, qb, qa, 1.0 / 3.0, 2.0 / 3.0)

    for f in range(2):
        flows = [depth_ref[:, lanes(t)] * (carry[2 + f][t] / levels) for t in range(tiles)]
        for t in range(tiles):
            flow_c[f, :, lanes(t)] = flows[t]
            all_flow[own, f, :, lanes(t)] = flows[t]
        flow_e[f] = jnp.where(lane < LANES // 2, flows[0], flows[-1])
    far(lambda o, side: far_copy(flow_kind, o, side).start())
    far(lambda o, side: far_wait(stat_kind, o, side))

    wide = tiles + 1

    def window(everything, edge, f):
        out = []
        for p in range(slots):
            line = [everything[p, f, :, lanes(t)] for t in range(tiles)]
            line.append(jnp.where(lane < LANES // 2, edge[1, p, f], edge[0, p, f]))
            out.append(line)
        return out

    def up(z, p, t):
        after = z[p + 1][t] if p + 1 < slots else zero
        return pltpu.roll(jnp.where(row < 1, after, z[p][t]), ROWS - 1, 0)

    def down(z, p, t):
        before = z[p - 1][t] if p > 0 else zero
        return pltpu.roll(jnp.where(row >= ROWS - 1, before, z[p][t]), 1, 0)

    def right(z, p, t):
        return pltpu.roll(jnp.where(lane < 1, z[p][(t + 1) % wide], z[p][t]), LANES - 1, 1)

    def left(z, p, t):
        return pltpu.roll(jnp.where(lane >= LANES - 1, z[p][(t - 1) % wide], z[p][t]), 1, 1)

    cells = [(p, t) for p in range(slots) for t in range(wide)]

    def grid(make):
        return [[make(p, t) for t in range(wide)] for p in range(slots)]

    x = window(all_stat, rim_stat, 0)
    wet = window(all_stat, rim_stat, 1)
    wet6 = grid(lambda p, t: wet[p][t] * (1.0 / 6.0))
    diag = grid(lambda p, t: wet[p][t] * SIGMA_SHIFT + (1.0 - wet[p][t]))

    def apply(e):
        w = grid(lambda p, t: wet[p][t] * e[p][t])
        a = grid(lambda p, t: up(w, p, t) + down(w, p, t))
        b = grid(lambda p, t: 4.0 * w[p][t] + a[p][t])
        return grid(
            lambda p, t: wet6[p][t]
            * ((20.0 * w[p][t] - 4.0 * a[p][t]) - (right(b, p, t) + left(b, p, t)))
            + diag[p][t] * e[p][t]
        )

    image = apply(x)

    far(lambda o, side: far_wait(flow_kind, o, side))
    fe = window(all_flow, rim_flow, 0)
    fn = window(all_flow, rim_flow, 1)

    def right_side(p, t):
        div = (up(fe, p, t) - down(fe, p, t)) * 0.5 + (right(fn, p, t) - left(fn, p, t)) * 0.5
        return wet[p][t] * (SIGMA_SHIFT * x[p][t] - DIVERGENCE_COEF * div)

    rhs = grid(right_side)
    r = grid(lambda p, t: rhs[p][t] - image[p][t])
    d = grid(lambda p, t: r[p][t] * (1.0 / CHEB_CENTER))
    keeps, gains = cheb_table(ITERS)
    for index in range(ITERS):
        x = grid(lambda p, t: x[p][t] + d[p][t])
        if index < ITERS - 1:
            image = apply(d)
            r = grid(lambda p, t: r[p][t] - image[p][t])
            d = grid(lambda p, t: keeps[index] * d[p][t] + gains[index] * r[p][t])

    for t in range(wide):
        xs[0, t] = zero
        xs[slots + 1, t] = zero
    for p, t in cells:
        xs[p + 1, t] = x[p][t]
    mine = [[xs[own + i, t] for t in range(wide)] for i in range(3)]
    slope_e = []
    slope_n = []
    for t in range(tiles):
        surface_out[:, lanes(t)] = mine[1][t]
        above = pltpu.roll(jnp.where(row < 1, mine[2][t], mine[1][t]), ROWS - 1, 0)
        below = pltpu.roll(jnp.where(row >= ROWS - 1, mine[0][t], mine[1][t]), 1, 0)
        slope_e.append((above - below) * 0.5)
        slope_n.append((right(mine, 1, t) - left(mine, 1, t)) * 0.5)

    def last(c, carry):
        for kk in range(CHUNK):
            k = c * CHUNK + kk
            for t in range(tiles):
                live = active[t] > k
                east_out[k, :, lanes(t)] = jnp.where(live, qa[0, k, :, lanes(t)] - slope_e[t], 0.0)
                north_out[k, :, lanes(t)] = jnp.where(live, qa[1, k, :, lanes(t)] - slope_n[t], 0.0)
        for stage in range(3):
            drain(stage, c)
        return carry

    lax.fori_loop(0, chunks, last, 0)
    far(lambda o, side: far_copy(stat_kind, o, side).wait_send())
    far(lambda o, side: far_copy(flow_kind, o, side).wait_send())


def solution(mesh):
    nx, ny = mesh.shape["gx"], mesh.shape["gy"]

    def local(east, north, salt, surface, depth, wet, active):
        levels, rows, width = east.shape
        assert rows == ROWS and width % LANES == 0 and levels % CHUNK == 0
        tiles = width // LANES
        chunks = levels // CHUNK
        groups = 3 * CHUNK // 4
        reach = min(nx - 1, -(-(ITERS + 2) // ROWS))
        slots = min(nx, 2 * reach + 1)
        f32 = jnp.float32
        vmem = pltpu.VMEM
        dma = pltpu.SemaphoreType.DMA
        block = pl.BlockSpec(memory_space=pltpu.VMEM)
        state = jax.ShapeDtypeStruct(east.shape, f32)
        span = 2 * reach + 1
        return pl.pallas_call(
            functools.partial(kernel, nx, ny, reach, slots),
            out_shape=(state, state, state, jax.ShapeDtypeStruct(surface.shape, f32)),
            in_specs=[block] * 7,
            out_specs=(block,) * 4,
            scratch_shapes=[
                vmem((3, levels, rows, width), f32),
                vmem((3, levels, rows, width), f32),
                vmem((3, levels, rows, width), f32),
                vmem((3, 2, chunks, groups, rows, width), f32),
                vmem((3, 2, chunks, groups, rows, width), f32),
                vmem((3, chunks, rows, LANES), f32),
                vmem((3, 2, chunks, rows, LANES), f32),
                vmem((2, rows, width), f32),
                vmem((2, rows, LANES), f32),
                vmem((2, rows, width), f32),
                vmem((2, rows, LANES), f32),
                vmem((slots, 2, rows, width), f32),
                vmem((2, slots, 2, rows, LANES), f32),
                vmem((slots, 2, rows, width), f32),
                vmem((2, slots, 2, rows, LANES), f32),
                vmem((slots + 2, tiles + 1, rows, LANES), f32),
                dma((3, 2, chunks)),
                dma((3, 2, chunks)),
                dma((3, 2, chunks)),
                dma((3, 2, chunks)),
                dma((span,)),
                dma((slots,)),
                dma((2, span)),
                dma((2, slots)),
                dma((span,)),
                dma((slots,)),
                dma((2, span)),
                dma((2, slots)),
            ],
            compiler_params=pltpu.CompilerParams(
                collective_id=0, has_side_effects=True, vmem_limit_bytes=48 * 1024 * 1024
            ),
        )(east, north, salt, surface, depth, wet, active)

    return jax.shard_map(
        local,
        mesh=mesh,
        in_specs=(
            P(None, "gx", "gy"),
            P(None, "gx", "gy"),
            P(None, "gx", "gy"),
            P("gx", "gy"),
            P("gx", "gy"),
            P("gx", "gy"),
            P("gx", "gy"),
        ),
        out_specs=(P(None, "gx", "gy"), P(None, "gx", "gy"), P(None, "gx", "gy"), P("gx", "gy")),
        check_vma=False,
    )
```

```python
import functools

import jax
import jax.numpy as jnp
from jax import lax
from jax.experimental import pallas as pl
from jax.experimental.pallas import tpu as pltpu
from jax.sharding import PartitionSpec as P

ITERS = 16

TIME_STEP = 0.2
CORIOLIS = 0.3
PRESS_COEF = 0.05
VISCOSITY = 0.1
DIFFUSIVITY = 0.1
SIGMA_SHIFT = 0.25
CHEB_CENTER = 3.625
CHEB_HALF = 3.375
DIVERGENCE_COEF = 8.0

ROWS = 8
LANES = 128
CHUNK = 8
MESH = pl.DeviceIdType.MESH


def cheb_table(count):
    first = CHEB_CENTER / CHEB_HALF
    ratio = 1.0 / first
    keeps = []
    gains = []
    for index in range(count):
        ratio_next = 1.0 / (2.0 * first - ratio)
        keeps.append(ratio_next * ratio)
        gains.append(2.0 * ratio_next / CHEB_HALF)
        ratio = ratio_next
    return (keeps, gains)


def kernel(
    nx, ny, reach, slots,
    east_hbm, north_hbm, salt_hbm, surface_hbm, depth_hbm, wet_hbm, active_hbm,
    state_out, slope_out, surface_out,
    east_ref, north_ref, salt_ref, surface_ref, depth_ref, wet_ref, active_ref, load_sem,
    q0, qa, qb, send_x, recv_x, send_y, recv_y,
    stat_c, stat_e, flow_c, flow_e, all_stat, rim_stat, all_flow, rim_flow, xs,
    x_send, x_recv, y_send, y_recv,
    stat_send, stat_recv, stat_rim_send, stat_rim_recv,
    flow_send, flow_recv, flow_rim_send, flow_rim_recv,
):
    gx = lax.axis_index("gx")
    gy = lax.axis_index("gy")
    levels = east_ref.shape[0]
    width = east_ref.shape[2]
    tiles = width // LANES
    chunks = levels // CHUNK
    groups = 3 * CHUNK // 4
    relative = slots < nx
    row = lax.broadcasted_iota(jnp.int32, (ROWS, LANES), 0)
    lane = lax.broadcasted_iota(jnp.int32, (ROWS, LANES), 1)
    pair = row // 2
    zero = jnp.zeros((ROWS, LANES), jnp.float32)

    def lanes(t):
        return slice(t * LANES, (t + 1) * LANES)

    def slot_in(owner, peer):
        return owner - peer + reach if relative else owner

    def inside(x, y):
        return jnp.logical_and(
            jnp.logical_and(x >= 0, x < nx), jnp.logical_and(y >= 0, y < ny)
        )

    loads = [
        pltpu.make_async_copy(source, target, load_sem.at[i])
        for i, (source, target) in enumerate((
            (active_hbm, active_ref), (wet_hbm, wet_ref), (east_hbm, east_ref),
            (north_hbm, north_ref), (salt_hbm, salt_ref), (surface_hbm, surface_ref),
            (depth_hbm, depth_ref),
        ))
    ]
    for load in loads:
        load.start()

    offsets = [o for o in range(-reach, reach + 1)]
    partners = [(o, side) for o in offsets for side in (-1, 0, 1) if (o, side) != (0, 0)]

    barrier = pltpu.get_barrier_semaphore()
    count = jnp.int32(0)
    for o, side in partners:
        there = inside(gx + o, gy + side)

        @pl.when(there)
        def _(o=o, side=side):
            pl.semaphore_signal(
                barrier, inc=1, device_id=(gx + o, gy + side), device_id_type=MESH
            )

        count = count + there.astype(jnp.int32)

    own = slot_in(gx, gx)

    for side, missing in ((0, gx == 0), (1, gx == nx - 1)):
        @pl.when(missing)
        def _(side=side):
            for stage in range(3):
                @pl.loop(0, chunks)
                def _(c, stage=stage):
                    recv_x[stage, side, c] = jnp.zeros((groups, ROWS, width), jnp.float32)

    for side, missing in ((0, gy == 0), (1, gy == ny - 1)):
        @pl.when(missing)
        def _(side=side):
            recv_y[:, side] = jnp.zeros((3, chunks, ROWS, LANES), jnp.float32)
            rim_stat[side] = jnp.zeros((slots, 2, ROWS, LANES), jnp.float32)
            rim_flow[side] = jnp.zeros((slots, 2, ROWS, LANES), jnp.float32)

    if relative:
        for o in offsets:
            @pl.when(jnp.logical_not(inside(gx + o, gy)))
            def _(o=o):
                for block in (all_stat, all_flow):
                    block[o + reach] = jnp.zeros((2, ROWS, width), jnp.float32)
                for block in (rim_stat, rim_flow):
                    for side in range(2):
                        block[side, o + reach] = jnp.zeros((2, ROWS, LANES), jnp.float32)

    def pack(state, stage, c):
        rim = zero
        for f in range(3):
            for half in range(CHUNK // 4):
                group = f * (CHUNK // 4) + half
                ups = [None] * tiles
                downs = [None] * tiles
                for m in range(4):
                    k = c * CHUNK + half * 4 + m
                    position = group * 4 + m
                    parts = [state[f, k, :, lanes(t)] for t in range(tiles)]
                    for t in range(tiles):
                        turned = parts[t] if m == 3 else pltpu.roll(parts[t], 2 * m + 2, 0)
                        if m == 0:
                            ups[t] = turned
                            downs[t] = turned
                        else:
                            ups[t] = jnp.where(pair == m, turned, ups[t])
                            downs[t] = jnp.where(pair == (m + 1) % 4, turned, downs[t])
                    ends = jnp.where(lane < LANES // 2, parts[0], parts[-1])
                    rim = jnp.where(
                        lane // 4 == position,
                        pltpu.roll(ends, (4 * position + 2) % LANES, 1),
                        rim,
                    )
                for t in range(tiles):
                    send_x[stage, 0, c, group, :, lanes(t)] = downs[t]
                    send_x[stage, 1, c, group, :, lanes(t)] = ups[t]
        send_y[stage, c] = rim

    def x_copy(stage, c, side):
        return pltpu.make_async_remote_copy(
            src_ref=send_x.at[stage, side, c],
            dst_ref=recv_x.at[stage, 1 - side, c],
            send_sem=x_send.at[stage, side, c],
            recv_sem=x_recv.at[stage, 1 - side, c],
            device_id=(gx + 2 * side - 1, gy),
            device_id_type=MESH,
        )

    def y_copy(stage, c, side):
        return pltpu.make_async_remote_copy(
            src_ref=send_y.at[stage, c],
            dst_ref=recv_y.at[stage, 1 - side, c],
            send_sem=y_send.at[stage, side, c],
            recv_sem=y_recv.at[stage, 1 - side, c],
            device_id=(gx, gy + 2 * side - 1),
            device_id_type=MESH,
        )

    near = [
        (x_copy, 0, gx > 0), (x_copy, 1, gx < nx - 1),
        (y_copy, 0, gy > 0), (y_copy, 1, gy < ny - 1),
    ]

    def launch(stage, c):
        for copy, side, there in near:
            @pl.when(there)
            def _(copy=copy, side=side):
                copy(stage, c, side).start()

    def arrive(stage, c):
        for copy, side, there in near:
            @pl.when(there)
            def _(copy=copy, side=side):
                copy(stage, c, 1 - side).wait_recv()

    def drain(stage, c):
        for copy, side, there in near:
            @pl.when(there)
            def _(copy=copy, side=side):
                copy(stage, c, side).wait_send()

    def far_copy(kind, o, side):
        block, rim, everything, edge, ss, rs, rss, rrs = kind
        slot = slot_in(gx, gx + o)
        if side == 0:
            return pltpu.make_async_remote_copy(
                src_ref=block, dst_ref=everything.at[slot],
                send_sem=ss.at[o + reach], recv_sem=rs.at[slot],
                device_id=(gx + o, gy), device_id_type=MESH,
            )
        to = (1 - side) // 2
        return pltpu.make_async_remote_copy(
            src_ref=rim, dst_ref=edge.at[to, slot],
            send_sem=rss.at[to, o + reach], recv_sem=rrs.at[to, slot],
            device_id=(gx + o, gy + side), device_id_type=MESH,
        )

    def far_wait(kind, o, side):
        block, rim, everything, edge, ss, rs, rss, rrs = kind
        slot = slot_in(gx + o, gx)
        if side == 0:
            pltpu.make_async_remote_copy(
                src_ref=block, dst_ref=everything.at[slot],
                send_sem=ss.at[o + reach], recv_sem=rs.at[slot],
                device_id=(gx + o, gy), device_id_type=MESH,
            ).wait_recv()
        else:
            at = (1 + side) // 2
            pltpu.make_async_remote_copy(
                src_ref=rim, dst_ref=edge.at[at, slot],
                send_sem=rss.at[at, o + reach], recv_sem=rrs.at[at, slot],
                device_id=(gx + o, gy + side), device_id_type=MESH,
            ).wait_recv()

    def far(action):
        for o, side in partners:
            @pl.when(inside(gx + o, gy + side))
            def _(o=o, side=side):
                action(o, side)

    stat_kind = (stat_c, stat_e, all_stat, rim_stat,
                 stat_send, stat_recv, stat_rim_send, stat_rim_recv)
    flow_kind = (flow_c, flow_e, all_flow, rim_flow,
                 flow_send, flow_recv, flow_rim_send, flow_rim_recv)

    for load in loads:
        load.wait()

    active = [active_ref[:, lanes(t)] * wet_ref[:, lanes(t)] for t in range(tiles)]
    inputs = (east_ref, north_ref, salt_ref)

    def mask_chunk(c):
        for kk in range(CHUNK):
            k = c * CHUNK + kk
            for t in range(tiles):
                live = active[t] > k
                for f in range(3):
                    q0[f, k, :, lanes(t)] = jnp.where(live, inputs[f][k, :, lanes(t)], 0.0)

    def first(c, carry):
        mask_chunk(c)
        pack(q0, 0, c)
        return carry

    lax.fori_loop(0, chunks, first, 0)

    stat_parts = (
        [surface_ref[:, lanes(t)] for t in range(tiles)],
        [wet_ref[:, lanes(t)].astype(jnp.float32) for t in range(tiles)],
    )
    for f in range(2):
        for t in range(tiles):
            stat_c[f, :, lanes(t)] = stat_parts[f][t]
            all_stat[own, f, :, lanes(t)] = stat_parts[f][t]
        stat_e[f] = jnp.where(lane < LANES // 2, stat_parts[f][0], stat_parts[f][-1])

    pl.semaphore_wait(barrier, count)

    def first_launch(c, carry):
        launch(0, c)
        return carry

    lax.fori_loop(0, chunks, first_launch, 0)
    far(lambda o, side: far_copy(stat_kind, o, side).start())

    def slope8(a, b, c, d):
        return 8.0 * (a - b) - (c - d)

    def run_stage(stage, src, dst, weight0, weight1):
        def body(c, carry):
            press_e, press_n, sum_e, sum_n = [list(x) for x in carry]
            arrive(stage, c)
            rims = jnp.where(lane % 4 < 2, recv_y[stage, 0, c], recv_y[stage, 1, c])
            for kk in range(CHUNK):
                k = c * CHUNK + kk
                fields = []
                for f in range(3):
                    position = f * CHUNK + kk
                    group, m = position // 4, position % 4
                    rim = pltpu.roll(rims, (-(4 * position + 2)) % LANES, 1)
                    parts = [src[f, k, :, lanes(t)] for t in range(tiles)]
                    per_tile = []
                    for t in range(tiles):
                        q = parts[t]
                        after = parts[t + 1] if t + 1 < tiles else rim
                        before = parts[t - 1] if t > 0 else rim
                        ends = jnp.where(
                            pair == m,
                            recv_x[stage, 0, c, group, :, lanes(t)],
                            recv_x[stage, 1, c, group, :, lanes(t)],
                        )
                        if m != 3:
                            ends = pltpu.roll(ends, (-(2 * m + 2)) % ROWS, 0)
                        e1 = pltpu.roll(jnp.where(row < 1, ends, q), ROWS - 1, 0)
                        e2 = pltpu.roll(jnp.where(row < 2, ends, q), ROWS - 2, 0)
                        w1 = pltpu.roll(jnp.where(row >= ROWS - 1, ends, q), 1, 0)
                        w2 = pltpu.roll(jnp.where(row >= ROWS - 2, ends, q), 2, 0)
                        n1 = pltpu.roll(jnp.where(lane < 1, after, q), LANES - 1, 1)
                        n2 = pltpu.roll(jnp.where(lane < 2, after, q), LANES - 2, 1)
                        s1 = pltpu.roll(jnp.where(lane >= LANES - 1, before, q), 1, 1)
                        s2 = pltpu.roll(jnp.where(lane >= LANES - 2, before, q), 2, 1)
                        dx = slope8(e1, w1, e2, w2)
                        dy = slope8(n1, s1, n2, s2)
                        lap = ((e1 + w1) + (n1 + s1)) - 4.0 * q
                        per_tile.append((q, dx, dy, lap))
                    fields.append(per_tile)
                for t in range(tiles):
                    live = active[t] > k
                    (u, ux, uy, ul), (v, vx, vy, vl), (s, sx, sy, sl) = [
                        fields[f][t] for f in range(3)
                    ]
                    press_e[t] = press_e[t] + sx
                    press_n[t] = press_n[t] + sy
                    um = u * (-1.0 / 12.0)
                    vm = v * (-1.0 / 12.0)
                    coef = -PRESS_COEF / 12.0
                    ru = (um * ux + vm * uy) + CORIOLIS * v + coef * press_e[t] + VISCOSITY * ul
                    rv = (um * vx + vm * vy) - CORIOLIS * u + coef * press_n[t] + VISCOSITY * vl
                    rs = (um * sx + vm * sy) + DIFFUSIVITY * sl
                    news = []
                    for f, (q, rate) in enumerate(((u, ru), (v, rv), (s, rs))):
                        new = q + TIME_STEP * rate
                        if weight0 is not None:
                            new = weight0 * q0[f, k, :, lanes(t)] + weight1 * new
                        new = jnp.where(live, new, 0.0)
                        news.append(new)
                        dst[f, k, :, lanes(t)] = new
                    if stage == 2:
                        sum_e[t] = sum_e[t] + news[0]
                        sum_n[t] = sum_n[t] + news[1]
            if stage < 2:
                pack(dst, stage + 1, c)
                launch(stage + 1, c)
            return (tuple(press_e), tuple(press_n), tuple(sum_e), tuple(sum_n))

        zeros = (zero,) * tiles
        return lax.fori_loop(0, chunks, body, (zeros, zeros, zeros, zeros))

    run_stage(0, q0, qa, None, None)
    run_stage(1, qa, qb, 0.75, 0.25)
    carry = run_stage(2, qb, state_out, 1.0 / 3.0, 2.0 / 3.0)

    for f in range(2):
        flows = [depth_ref[:, lanes(t)] * (carry[2 + f][t] / levels) for t in range(tiles)]
        for t in range(tiles):
            flow_c[f, :, lanes(t)] = flows[t]
            all_flow[own, f, :, lanes(t)] = flows[t]
        flow_e[f] = jnp.where(lane < LANES // 2, flows[0], flows[-1])
    far(lambda o, side: far_copy(flow_kind, o, side).start())
    far(lambda o, side: far_wait(stat_kind, o, side))

    wide = tiles + 1

    def window(everything, edge, f):
        out = []
        for p in range(slots):
            line = [everything[p, f, :, lanes(t)] for t in range(tiles)]
            line.append(jnp.where(lane < LANES // 2, edge[1, p, f], edge[0, p, f]))
            out.append(line)
        return out

    def up(z, p, t):
        after = z[p + 1][t] if p + 1 < slots else zero
        return pltpu.roll(jnp.where(row < 1, after, z[p][t]), ROWS - 1, 0)

    def down(z, p, t):
        before = z[p - 1][t] if p > 0 else zero
        return pltpu.roll(jnp.where(row >= ROWS - 1, before, z[p][t]), 1, 0)

    def right(z, p, t):
        return pltpu.roll(jnp.where(lane < 1, z[p][(t + 1) % wide], z[p][t]), LANES - 1, 1)

    def left(z, p, t):
        return pltpu.roll(jnp.where(lane >= LANES - 1, z[p][(t - 1) % wide], z[p][t]), 1, 1)

    cells = [(p, t) for p in range(slots) for t in range(wide)]

    def grid(make):
        return [[make(p, t) for t in range(wide)] for p in range(slots)]

    x = window(all_stat, rim_stat, 0)
    wet = window(all_stat, rim_stat, 1)
    wet6 = grid(lambda p, t: wet[p][t] * (1.0 / 6.0))
    diag = grid(lambda p, t: wet[p][t] * SIGMA_SHIFT + (1.0 - wet[p][t]))

    def apply(e):
        w = grid(lambda p, t: wet[p][t] * e[p][t])
        a = grid(lambda p, t: up(w, p, t) + down(w, p, t))
        b = grid(lambda p, t: 4.0 * w[p][t] + a[p][t])
        return grid(
            lambda p, t: wet6[p][t]
            * ((20.0 * w[p][t] - 4.0 * a[p][t]) - (right(b, p, t) + left(b, p, t)))
            + diag[p][t] * e[p][t]
        )

    image = apply(x)

    far(lambda o, side: far_wait(flow_kind, o, side))
    fe = window(all_flow, rim_flow, 0)
    fn = window(all_flow, rim_flow, 1)

    def right_side(p, t):
        div = (up(fe, p, t) - down(fe, p, t)) * 0.5 + (right(fn, p, t) - left(fn, p, t)) * 0.5
        return wet[p][t] * (SIGMA_SHIFT * x[p][t] - DIVERGENCE_COEF * div)

    rhs = grid(right_side)
    r = grid(lambda p, t: rhs[p][t] - image[p][t])
    d = grid(lambda p, t: r[p][t] * (1.0 / CHEB_CENTER))
    keeps, gains = cheb_table(ITERS)
    for index in range(ITERS):
        x = grid(lambda p, t: x[p][t] + d[p][t])
        if index < ITERS - 1:
            image = apply(d)
            r = grid(lambda p, t: r[p][t] - image[p][t])
            d = grid(lambda p, t: keeps[index] * d[p][t] + gains[index] * r[p][t])

    for t in range(wide):
        xs[0, t] = zero
        xs[slots + 1, t] = zero
    for p, t in cells:
        xs[p + 1, t] = x[p][t]
    mine = [[xs[own + i, t] for t in range(wide)] for i in range(3)]
    for t in range(tiles):
        surface_out[:, lanes(t)] = mine[1][t]
        above = pltpu.roll(jnp.where(row < 1, mine[2][t], mine[1][t]), ROWS - 1, 0)
        below = pltpu.roll(jnp.where(row >= ROWS - 1, mine[0][t], mine[1][t]), 1, 0)
        slope_out[0, :, lanes(t)] = (above - below) * 0.5
        slope_out[1, :, lanes(t)] = (right(mine, 1, t) - left(mine, 1, t)) * 0.5

    def last(c, carry):
        for stage in range(3):
            drain(stage, c)
        return carry

    lax.fori_loop(0, chunks, last, 0)
    far(lambda o, side: far_copy(stat_kind, o, side).wait_send())
    far(lambda o, side: far_copy(flow_kind, o, side).wait_send())


def finish(
    state_ref, slope_ref, surface_ref, wet_ref, active_ref,
    east_out, north_out, salt_out, surface_out, held, sems,
):
    early = (
        pltpu.make_async_copy(state_ref.at[2], salt_out, sems.at[0]),
        pltpu.make_async_copy(surface_ref, surface_out, sems.at[1]),
    )
    for copy in early:
        copy.start()
    levels = held.shape[1]
    active = active_ref[...] * wet_ref[...]
    slopes = (slope_ref[0], slope_ref[1])
    for f in range(2):
        for k in range(levels):
            held[f, k] = jnp.where(active > k, state_ref[f, k] - slopes[f], 0.0)
        pltpu.make_async_copy(held.at[f], (east_out, north_out)[f], sems.at[2 + f]).start()
    for f in range(2):
        pltpu.make_async_copy(held.at[f], (east_out, north_out)[f], sems.at[2 + f]).wait()
    for copy in early:
        copy.wait()


def solution(mesh):
    nx, ny = mesh.shape["gx"], mesh.shape["gy"]

    def local(east, north, salt, surface, depth, wet, active):
        levels, rows, width = east.shape
        assert rows == ROWS and width % LANES == 0 and levels % CHUNK == 0
        tiles = width // LANES
        chunks = levels // CHUNK
        groups = 3 * CHUNK // 4
        reach = min(nx - 1, -(-(ITERS + 2) // ROWS))
        slots = min(nx, 2 * reach + 1)
        f32 = jnp.float32
        vmem = pltpu.VMEM
        dma = pltpu.SemaphoreType.DMA
        block = pl.BlockSpec(memory_space=pltpu.VMEM)
        state = jax.ShapeDtypeStruct(east.shape, f32)
        span = 2 * reach + 1
        hbm = pl.BlockSpec(memory_space=pltpu.HBM)
        state3, slopes, surface_next = pl.pallas_call(
            functools.partial(kernel, nx, ny, reach, slots),
            out_shape=(
                jax.ShapeDtypeStruct((3,) + east.shape, f32),
                jax.ShapeDtypeStruct((2,) + surface.shape, f32),
                jax.ShapeDtypeStruct(surface.shape, f32),
            ),
            in_specs=[hbm] * 7,
            out_specs=(block,) * 3,
            scratch_shapes=[
                vmem(east.shape, f32),
                vmem(east.shape, f32),
                vmem(east.shape, f32),
                vmem(surface.shape, f32),
                vmem(surface.shape, f32),
                vmem(surface.shape, jnp.int32),
                vmem(surface.shape, jnp.int32),
                dma((7,)),
                vmem((3, levels, rows, width), f32),
                vmem((3, levels, rows, width), f32),
                vmem((3, levels, rows, width), f32),
                vmem((3, 2, chunks, groups, rows, width), f32),
                vmem((3, 2, chunks, groups, rows, width), f32),
                vmem((3, chunks, rows, LANES), f32),
                vmem((3, 2, chunks, rows, LANES), f32),
                vmem((2, rows, width), f32),
                vmem((2, rows, LANES), f32),
                vmem((2, rows, width), f32),
                vmem((2, rows, LANES), f32),
                vmem((slots, 2, rows, width), f32),
                vmem((2, slots, 2, rows, LANES), f32),
                vmem((slots, 2, rows, width), f32),
                vmem((2, slots, 2, rows, LANES), f32),
                vmem((slots + 2, tiles + 1, rows, LANES), f32),
                dma((3, 2, chunks)),
                dma((3, 2, chunks)),
                dma((3, 2, chunks)),
                dma((3, 2, chunks)),
                dma((span,)),
                dma((slots,)),
                dma((2, span)),
                dma((2, slots)),
                dma((span,)),
                dma((slots,)),
                dma((2, span)),
                dma((2, slots)),
            ],
            compiler_params=pltpu.CompilerParams(
                collective_id=0, has_side_effects=True, vmem_limit_bytes=48 * 1024 * 1024
            ),
        )(*[
            pltpu.with_memory_space_constraint(z, pltpu.HBM)
            for z in (east, north, salt, surface, depth, wet, active)
        ])
        return pl.pallas_call(
            finish,
            out_shape=(state, state, state, jax.ShapeDtypeStruct(surface.shape, f32)),
            in_specs=[block] * 5,
            out_specs=(hbm,) * 4,
            scratch_shapes=[vmem((2,) + east.shape, f32), dma((4,))],
            compiler_params=pltpu.CompilerParams(vmem_limit_bytes=8 * 1024 * 1024),
        )(state3, slopes, surface_next, wet, active)

    return jax.shard_map(
        local,
        mesh=mesh,
        in_specs=(
            P(None, "gx", "gy"),
            P(None, "gx", "gy"),
            P(None, "gx", "gy"),
            P("gx", "gy"),
            P("gx", "gy"),
            P("gx", "gy"),
            P("gx", "gy"),
        ),
        out_specs=(P(None, "gx", "gy"), P(None, "gx", "gy"), P(None, "gx", "gy"), P("gx", "gy")),
        check_vma=False,
    )
```

```python
import functools

import jax
import jax.numpy as jnp
from jax import lax
from jax.experimental import pallas as pl
from jax.experimental.pallas import tpu as pltpu
from jax.sharding import PartitionSpec as P

ITERS = 16

TIME_STEP = 0.2
CORIOLIS = 0.3
PRESS_COEF = 0.05
VISCOSITY = 0.1
DIFFUSIVITY = 0.1
SIGMA_SHIFT = 0.25
CHEB_CENTER = 3.625
CHEB_HALF = 3.375
DIVERGENCE_COEF = 8.0

ROWS = 8
LANES = 128
CHUNK = 8
MESH = pl.DeviceIdType.MESH


def cheb_table(count):
    first = CHEB_CENTER / CHEB_HALF
    ratio = 1.0 / first
    keeps = []
    gains = []
    for index in range(count):
        ratio_next = 1.0 / (2.0 * first - ratio)
        keeps.append(ratio_next * ratio)
        gains.append(2.0 * ratio_next / CHEB_HALF)
        ratio = ratio_next
    return (keeps, gains)


def kernel(
    nx, ny, reach, slots,
    east_hbm, north_hbm, salt_hbm, surface_hbm, depth_hbm, wet_hbm, active_hbm,
    state_out, slope_out, surface_out,
    east_ref, north_ref, salt_ref, surface_ref, depth_ref, wet_ref, active_ref, load_sem,
    shifts, moved, q0, qa, qb, send_x, recv_x, send_y, recv_y,
    stat_c, stat_e, flow_c, flow_e, all_stat, rim_stat, all_flow, rim_flow, xs,
    x_send, x_recv, y_send, y_recv,
    stat_send, stat_recv, stat_rim_send, stat_rim_recv,
    flow_send, flow_recv, flow_rim_send, flow_rim_recv,
):
    gx = lax.axis_index("gx")
    gy = lax.axis_index("gy")
    levels = east_ref.shape[0]
    width = east_ref.shape[2]
    tiles = width // LANES
    chunks = levels // CHUNK
    groups = 3 * CHUNK // 4
    relative = slots < nx
    row = lax.broadcasted_iota(jnp.int32, (ROWS, LANES), 0)
    lane = lax.broadcasted_iota(jnp.int32, (ROWS, LANES), 1)
    pair = row // 2
    zero = jnp.zeros((ROWS, LANES), jnp.float32)

    def lanes(t):
        return slice(t * LANES, (t + 1) * LANES)

    def slot_in(owner, peer):
        return owner - peer + reach if relative else owner

    def inside(x, y):
        return jnp.logical_and(
            jnp.logical_and(x >= 0, x < nx), jnp.logical_and(y >= 0, y < ny)
        )

    loads = [
        pltpu.make_async_copy(source, target, load_sem.at[i])
        for i, (source, target) in enumerate((
            (active_hbm, active_ref), (wet_hbm, wet_ref), (east_hbm, east_ref),
            (north_hbm, north_ref), (salt_hbm, salt_ref), (surface_hbm, surface_ref),
            (depth_hbm, depth_ref),
        ))
    ]
    for load in loads:
        load.start()

    offsets = [o for o in range(-reach, reach + 1)]
    partners = [(o, side) for o in offsets for side in (-1, 0, 1) if (o, side) != (0, 0)]

    barrier = pltpu.get_barrier_semaphore()
    count = jnp.int32(0)
    for o, side in partners:
        there = inside(gx + o, gy + side)

        @pl.when(there)
        def _(o=o, side=side):
            pl.semaphore_signal(
                barrier, inc=1, device_id=(gx + o, gy + side), device_id_type=MESH
            )

        count = count + there.astype(jnp.int32)

    own = slot_in(gx, gx)

    for side, missing in ((0, gx == 0), (1, gx == nx - 1)):
        @pl.when(missing)
        def _(side=side):
            for stage in range(3):
                @pl.loop(0, chunks)
                def _(c, stage=stage):
                    recv_x[stage, side, c] = jnp.zeros((groups, ROWS, width), jnp.float32)

    for side, missing in ((0, gy == 0), (1, gy == ny - 1)):
        @pl.when(missing)
        def _(side=side):
            recv_y[:, side] = jnp.zeros((3, chunks, ROWS, LANES), jnp.float32)
            rim_stat[side] = jnp.zeros((slots, 2, ROWS, LANES), jnp.float32)
            rim_flow[side] = jnp.zeros((slots, 2, ROWS, LANES), jnp.float32)

    if relative:
        for o in offsets:
            @pl.when(jnp.logical_not(inside(gx + o, gy)))
            def _(o=o):
                for block in (all_stat, all_flow):
                    block[o + reach] = jnp.zeros((2, ROWS, width), jnp.float32)
                for block in (rim_stat, rim_flow):
                    for side in range(2):
                        block[side, o + reach] = jnp.zeros((2, ROWS, LANES), jnp.float32)

    def pack(state, stage, c):
        rim = zero
        for f in range(3):
            for half in range(CHUNK // 4):
                group = f * (CHUNK // 4) + half
                ups = [None] * tiles
                downs = [None] * tiles
                for m in range(4):
                    k = c * CHUNK + half * 4 + m
                    position = group * 4 + m
                    parts = [state[f, k, :, lanes(t)] for t in range(tiles)]
                    for t in range(tiles):
                        turned = parts[t] if m == 3 else pltpu.roll(parts[t], 2 * m + 2, 0)
                        if m == 0:
                            ups[t] = turned
                            downs[t] = turned
                        else:
                            ups[t] = jnp.where(pair == m, turned, ups[t])
                            downs[t] = jnp.where(pair == (m + 1) % 4, turned, downs[t])
                    ends = jnp.where(lane < LANES // 2, parts[0], parts[-1])
                    rim = jnp.where(
                        lane // 4 == position,
                        pltpu.roll(ends, (4 * position + 2) % LANES, 1),
                        rim,
                    )
                for t in range(tiles):
                    send_x[stage, 0, c, group, :, lanes(t)] = downs[t]
                    send_x[stage, 1, c, group, :, lanes(t)] = ups[t]
        send_y[stage, c] = rim

    def x_copy(stage, c, side):
        return pltpu.make_async_remote_copy(
            src_ref=send_x.at[stage, side, c],
            dst_ref=recv_x.at[stage, 1 - side, c],
            send_sem=x_send.at[stage, side, c],
            recv_sem=x_recv.at[stage, 1 - side, c],
            device_id=(gx + 2 * side - 1, gy),
            device_id_type=MESH,
        )

    def y_copy(stage, c, side):
        return pltpu.make_async_remote_copy(
            src_ref=send_y.at[stage, c],
            dst_ref=recv_y.at[stage, 1 - side, c],
            send_sem=y_send.at[stage, side, c],
            recv_sem=y_recv.at[stage, 1 - side, c],
            device_id=(gx, gy + 2 * side - 1),
            device_id_type=MESH,
        )

    near = [
        (x_copy, 0, gx > 0), (x_copy, 1, gx < nx - 1),
        (y_copy, 0, gy > 0), (y_copy, 1, gy < ny - 1),
    ]

    def launch(stage, c):
        for copy, side, there in near:
            @pl.when(there)
            def _(copy=copy, side=side):
                copy(stage, c, side).start()

    def arrive(stage, c):
        for copy, side, there in near:
            @pl.when(there)
            def _(copy=copy, side=side):
                copy(stage, c, 1 - side).wait_recv()

    def drain(stage, c):
        for copy, side, there in near:
            @pl.when(there)
            def _(copy=copy, side=side):
                copy(stage, c, side).wait_send()

    def far_copy(kind, o, side):
        block, rim, everything, edge, ss, rs, rss, rrs = kind
        slot = slot_in(gx, gx + o)
        if side == 0:
            return pltpu.make_async_remote_copy(
                src_ref=block, dst_ref=everything.at[slot],
                send_sem=ss.at[o + reach], recv_sem=rs.at[slot],
                device_id=(gx + o, gy), device_id_type=MESH,
            )
        to = (1 - side) // 2
        return pltpu.make_async_remote_copy(
            src_ref=rim, dst_ref=edge.at[to, slot],
            send_sem=rss.at[to, o + reach], recv_sem=rrs.at[to, slot],
            device_id=(gx + o, gy + side), device_id_type=MESH,
        )

    def far_wait(kind, o, side):
        block, rim, everything, edge, ss, rs, rss, rrs = kind
        slot = slot_in(gx + o, gx)
        if side == 0:
            pltpu.make_async_remote_copy(
                src_ref=block, dst_ref=everything.at[slot],
                send_sem=ss.at[o + reach], recv_sem=rs.at[slot],
                device_id=(gx + o, gy), device_id_type=MESH,
            ).wait_recv()
        else:
            at = (1 + side) // 2
            pltpu.make_async_remote_copy(
                src_ref=rim, dst_ref=edge.at[at, slot],
                send_sem=rss.at[at, o + reach], recv_sem=rrs.at[at, slot],
                device_id=(gx + o, gy + side), device_id_type=MESH,
            ).wait_recv()

    def far(action):
        for o, side in partners:
            @pl.when(inside(gx + o, gy + side))
            def _(o=o, side=side):
                action(o, side)

    stat_kind = (stat_c, stat_e, all_stat, rim_stat,
                 stat_send, stat_recv, stat_rim_send, stat_rim_recv)
    flow_kind = (flow_c, flow_e, all_flow, rim_flow,
                 flow_send, flow_recv, flow_rim_send, flow_rim_recv)

    source = lax.broadcasted_iota(jnp.int32, (width, width), 0)
    target = lax.broadcasted_iota(jnp.int32, (width, width), 1)
    step = source - target
    one = jnp.abs(step) == 1
    sign = jnp.where(step > 0, 1.0, -1.0)
    slope = jnp.where(one, 8.0 * sign, jnp.where(jnp.abs(step) == 2, -sign, 0.0))
    shifts[:, :width] = slope.astype(jnp.bfloat16)
    shifts[:, width:] = jnp.where(one, 1.0, 0.0).astype(jnp.bfloat16)

    def move_chunk(src, c):
        for f in range(3):
            whole = src[f, pl.ds(c * CHUNK, CHUNK)].reshape(CHUNK * ROWS, width)
            high = whole.astype(jnp.bfloat16)
            rest = whole - high.astype(jnp.float32)
            middle = rest.astype(jnp.bfloat16)
            low = (rest - middle.astype(jnp.float32)).astype(jnp.bfloat16)
            total = jnp.dot(low, shifts[...], preferred_element_type=jnp.float32)
            total = total + jnp.dot(middle, shifts[...], preferred_element_type=jnp.float32)
            total = total + jnp.dot(high, shifts[...], preferred_element_type=jnp.float32)
            moved[f] = total.reshape(CHUNK, ROWS, 2 * width)

    for load in loads:
        load.wait()

    active = [active_ref[:, lanes(t)] * wet_ref[:, lanes(t)] for t in range(tiles)]
    inputs = (east_ref, north_ref, salt_ref)

    def mask_chunk(c):
        for kk in range(CHUNK):
            k = c * CHUNK + kk
            for t in range(tiles):
                live = active[t] > k
                for f in range(3):
                    q0[f, k, :, lanes(t)] = jnp.where(live, inputs[f][k, :, lanes(t)], 0.0)

    def first(c, carry):
        mask_chunk(c)
        pack(q0, 0, c)
        return carry

    lax.fori_loop(0, chunks, first, 0)

    stat_parts = (
        [surface_ref[:, lanes(t)] for t in range(tiles)],
        [wet_ref[:, lanes(t)].astype(jnp.float32) for t in range(tiles)],
    )
    for f in range(2):
        for t in range(tiles):
            stat_c[f, :, lanes(t)] = stat_parts[f][t]
            all_stat[own, f, :, lanes(t)] = stat_parts[f][t]
        stat_e[f] = jnp.where(lane < LANES // 2, stat_parts[f][0], stat_parts[f][-1])

    pl.semaphore_wait(barrier, count)

    def first_launch(c, carry):
        launch(0, c)
        return carry

    lax.fori_loop(0, chunks, first_launch, 0)
    far(lambda o, side: far_copy(stat_kind, o, side).start())

    def slope8(a, b, c, d):
        return 8.0 * (a - b) - (c - d)

    def run_stage(stage, src, dst, weight0, weight1):
        def body(c, carry):
            press_e, press_n, sum_e, sum_n = [list(x) for x in carry]
            arrive(stage, c)
            rims = jnp.where(lane % 4 < 2, recv_y[stage, 0, c], recv_y[stage, 1, c])
            move_chunk(src, c)
            r1, r2 = pltpu.roll(rims, LANES - 1, 1), pltpu.roll(rims, LANES - 2, 1)
            l1, l2 = pltpu.roll(rims, 1, 1), pltpu.roll(rims, 2, 1)
            quarter = lane % 4
            rim_slope = jnp.where(
                quarter < 2,
                jnp.where(quarter == 0, -r2, 8.0 * r1 - r2),
                jnp.where(quarter == 2, l2 - 8.0 * l1, l2),
            )
            rim_sum = jnp.where(quarter == 1, r1, jnp.where(quarter == 2, l1, 0.0))
            for kk in range(CHUNK):
                k = c * CHUNK + kk
                fields = []
                for f in range(3):
                    position = f * CHUNK + kk
                    group, m = position // 4, position % 4
                    extra_slope = pltpu.roll(rim_slope, (-(4 * position + 2)) % LANES, 1)
                    extra_sum = pltpu.roll(rim_sum, (-(4 * position + 2)) % LANES, 1)
                    parts = [src[f, k, :, lanes(t)] for t in range(tiles)]
                    per_tile = []
                    for t in range(tiles):
                        q = parts[t]
                        ends = jnp.where(
                            pair == m,
                            recv_x[stage, 0, c, group, :, lanes(t)],
                            recv_x[stage, 1, c, group, :, lanes(t)],
                        )
                        if m != 3:
                            ends = pltpu.roll(ends, (-(2 * m + 2)) % ROWS, 0)
                        e1 = pltpu.roll(jnp.where(row < 1, ends, q), ROWS - 1, 0)
                        e2 = pltpu.roll(jnp.where(row < 2, ends, q), ROWS - 2, 0)
                        w1 = pltpu.roll(jnp.where(row >= ROWS - 1, ends, q), 1, 0)
                        w2 = pltpu.roll(jnp.where(row >= ROWS - 2, ends, q), 2, 0)
                        dy = moved[f, kk, :, lanes(t)]
                        sides = moved[f, kk, :, lanes(tiles + t)]
                        if t == 0:
                            dy = dy + jnp.where(lane < 2, extra_slope, 0.0)
                            sides = sides + jnp.where(lane < 2, extra_sum, 0.0)
                        if t == tiles - 1:
                            dy = dy + jnp.where(lane >= LANES - 2, extra_slope, 0.0)
                            sides = sides + jnp.where(lane >= LANES - 2, extra_sum, 0.0)
                        dx = slope8(e1, w1, e2, w2)
                        lap = ((e1 + w1) + sides) - 4.0 * q
                        per_tile.append((q, dx, dy, lap))
                    fields.append(per_tile)
                for t in range(tiles):
                    live = active[t] > k
                    (u, ux, uy, ul), (v, vx, vy, vl), (s, sx, sy, sl) = [
                        fields[f][t] for f in range(3)
                    ]
                    press_e[t] = press_e[t] + sx
                    press_n[t] = press_n[t] + sy
                    um = u * (-1.0 / 12.0)
                    vm = v * (-1.0 / 12.0)
                    coef = -PRESS_COEF / 12.0
                    ru = (um * ux + vm * uy) + CORIOLIS * v + coef * press_e[t] + VISCOSITY * ul
                    rv = (um * vx + vm * vy) - CORIOLIS * u + coef * press_n[t] + VISCOSITY * vl
                    rs = (um * sx + vm * sy) + DIFFUSIVITY * sl
                    news = []
                    for f, (q, rate) in enumerate(((u, ru), (v, rv), (s, rs))):
                        new = q + TIME_STEP * rate
                        if weight0 is not None:
                            new = weight0 * q0[f, k, :, lanes(t)] + weight1 * new
                        new = jnp.where(live, new, 0.0)
                        news.append(new)
                        dst[f, k, :, lanes(t)] = new
                    if stage == 2:
                        sum_e[t] = sum_e[t] + news[0]
                        sum_n[t] = sum_n[t] + news[1]
            if stage < 2:
                pack(dst, stage + 1, c)
                launch(stage + 1, c)
            return (tuple(press_e), tuple(press_n), tuple(sum_e), tuple(sum_n))

        zeros = (zero,) * tiles
        return lax.fori_loop(0, chunks, body, (zeros, zeros, zeros, zeros))

    run_stage(0, q0, qa, None, None)
    run_stage(1, qa, qb, 0.75, 0.25)
    carry = run_stage(2, qb, state_out, 1.0 / 3.0, 2.0 / 3.0)

    for f in range(2):
        flows = [depth_ref[:, lanes(t)] * (carry[2 + f][t] / levels) for t in range(tiles)]
        for t in range(tiles):
            flow_c[f, :, lanes(t)] = flows[t]
            all_flow[own, f, :, lanes(t)] = flows[t]
        flow_e[f] = jnp.where(lane < LANES // 2, flows[0], flows[-1])
    far(lambda o, side: far_copy(flow_kind, o, side).start())
    far(lambda o, side: far_wait(stat_kind, o, side))

    wide = tiles + 1

    def window(everything, edge, f):
        out = []
        for p in range(slots):
            line = [everything[p, f, :, lanes(t)] for t in range(tiles)]
            line.append(jnp.where(lane < LANES // 2, edge[1, p, f], edge[0, p, f]))
            out.append(line)
        return out

    def up(z, p, t):
        after = z[p + 1][t] if p + 1 < slots else zero
        return pltpu.roll(jnp.where(row < 1, after, z[p][t]), ROWS - 1, 0)

    def down(z, p, t):
        before = z[p - 1][t] if p > 0 else zero
        return pltpu.roll(jnp.where(row >= ROWS - 1, before, z[p][t]), 1, 0)

    def right(z, p, t):
        return pltpu.roll(jnp.where(lane < 1, z[p][(t + 1) % wide], z[p][t]), LANES - 1, 1)

    def left(z, p, t):
        return pltpu.roll(jnp.where(lane >= LANES - 1, z[p][(t - 1) % wide], z[p][t]), 1, 1)

    cells = [(p, t) for p in range(slots) for t in range(wide)]

    def grid(make):
        return [[make(p, t) for t in range(wide)] for p in range(slots)]

    x = window(all_stat, rim_stat, 0)
    wet = window(all_stat, rim_stat, 1)
    wet6 = grid(lambda p, t: wet[p][t] * (1.0 / 6.0))
    diag = grid(lambda p, t: wet[p][t] * SIGMA_SHIFT + (1.0 - wet[p][t]))

    def apply(e):
        w = grid(lambda p, t: wet[p][t] * e[p][t])
        a = grid(lambda p, t: up(w, p, t) + down(w, p, t))
        b = grid(lambda p, t: 4.0 * w[p][t] + a[p][t])
        return grid(
            lambda p, t: wet6[p][t]
            * ((20.0 * w[p][t] - 4.0 * a[p][t]) - (right(b, p, t) + left(b, p, t)))
            + diag[p][t] * e[p][t]
        )

    image = apply(x)

    far(lambda o, side: far_wait(flow_kind, o, side))
    fe = window(all_flow, rim_flow, 0)
    fn = window(all_flow, rim_flow, 1)

    def right_side(p, t):
        div = (up(fe, p, t) - down(fe, p, t)) * 0.5 + (right(fn, p, t) - left(fn, p, t)) * 0.5
        return wet[p][t] * (SIGMA_SHIFT * x[p][t] - DIVERGENCE_COEF * div)

    rhs = grid(right_side)
    r = grid(lambda p, t: rhs[p][t] - image[p][t])
    d = grid(lambda p, t: r[p][t] * (1.0 / CHEB_CENTER))
    keeps, gains = cheb_table(ITERS)
    for index in range(ITERS):
        x = grid(lambda p, t: x[p][t] + d[p][t])
        if index < ITERS - 1:
            image = apply(d)
            r = grid(lambda p, t: r[p][t] - image[p][t])
            d = grid(lambda p, t: keeps[index] * d[p][t] + gains[index] * r[p][t])

    for t in range(wide):
        xs[0, t] = zero
        xs[slots + 1, t] = zero
    for p, t in cells:
        xs[p + 1, t] = x[p][t]
    mine = [[xs[own + i, t] for t in range(wide)] for i in range(3)]
    for t in range(tiles):
        surface_out[:, lanes(t)] = mine[1][t]
        above = pltpu.roll(jnp.where(row < 1, mine[2][t], mine[1][t]), ROWS - 1, 0)
        below = pltpu.roll(jnp.where(row >= ROWS - 1, mine[0][t], mine[1][t]), 1, 0)
        slope_out[0, :, lanes(t)] = (above - below) * 0.5
        slope_out[1, :, lanes(t)] = (right(mine, 1, t) - left(mine, 1, t)) * 0.5

    def last(c, carry):
        for stage in range(3):
            drain(stage, c)
        return carry

    lax.fori_loop(0, chunks, last, 0)
    far(lambda o, side: far_copy(stat_kind, o, side).wait_send())
    far(lambda o, side: far_copy(flow_kind, o, side).wait_send())


def finish(
    state_ref, slope_ref, surface_ref, wet_ref, active_ref,
    east_out, north_out, salt_out, surface_out, held, sems,
):
    early = (
        pltpu.make_async_copy(state_ref.at[2], salt_out, sems.at[0]),
        pltpu.make_async_copy(surface_ref, surface_out, sems.at[1]),
    )
    for copy in early:
        copy.start()
    levels = held.shape[1]
    active = active_ref[...] * wet_ref[...]
    slopes = (slope_ref[0], slope_ref[1])
    for f in range(2):
        for k in range(levels):
            held[f, k] = jnp.where(active > k, state_ref[f, k] - slopes[f], 0.0)
        pltpu.make_async_copy(held.at[f], (east_out, north_out)[f], sems.at[2 + f]).start()
    for f in range(2):
        pltpu.make_async_copy(held.at[f], (east_out, north_out)[f], sems.at[2 + f]).wait()
    for copy in early:
        copy.wait()


def solution(mesh):
    nx, ny = mesh.shape["gx"], mesh.shape["gy"]

    def local(east, north, salt, surface, depth, wet, active):
        levels, rows, width = east.shape
        assert rows == ROWS and width % LANES == 0 and levels % CHUNK == 0
        tiles = width // LANES
        chunks = levels // CHUNK
        groups = 3 * CHUNK // 4
        reach = min(nx - 1, -(-(ITERS + 2) // ROWS))
        slots = min(nx, 2 * reach + 1)
        f32 = jnp.float32
        vmem = pltpu.VMEM
        dma = pltpu.SemaphoreType.DMA
        block = pl.BlockSpec(memory_space=pltpu.VMEM)
        state = jax.ShapeDtypeStruct(east.shape, f32)
        span = 2 * reach + 1
        hbm = pl.BlockSpec(memory_space=pltpu.HBM)
        state3, slopes, surface_next = pl.pallas_call(
            functools.partial(kernel, nx, ny, reach, slots),
            out_shape=(
                jax.ShapeDtypeStruct((3,) + east.shape, f32),
                jax.ShapeDtypeStruct((2,) + surface.shape, f32),
                jax.ShapeDtypeStruct(surface.shape, f32),
            ),
            in_specs=[hbm] * 7,
            out_specs=(block,) * 3,
            scratch_shapes=[
                vmem(east.shape, f32),
                vmem(east.shape, f32),
                vmem(east.shape, f32),
                vmem(surface.shape, f32),
                vmem(surface.shape, f32),
                vmem(surface.shape, jnp.int32),
                vmem(surface.shape, jnp.int32),
                dma((7,)),
                vmem((width, 2 * width), jnp.bfloat16),
                vmem((3, CHUNK, rows, 2 * width), f32),
                vmem((3, levels, rows, width), f32),
                vmem((3, levels, rows, width), f32),
                vmem((3, levels, rows, width), f32),
                vmem((3, 2, chunks, groups, rows, width), f32),
                vmem((3, 2, chunks, groups, rows, width), f32),
                vmem((3, chunks, rows, LANES), f32),
                vmem((3, 2, chunks, rows, LANES), f32),
                vmem((2, rows, width), f32),
                vmem((2, rows, LANES), f32),
                vmem((2, rows, width), f32),
                vmem((2, rows, LANES), f32),
                vmem((slots, 2, rows, width), f32),
                vmem((2, slots, 2, rows, LANES), f32),
                vmem((slots, 2, rows, width), f32),
                vmem((2, slots, 2, rows, LANES), f32),
                vmem((slots + 2, tiles + 1, rows, LANES), f32),
                dma((3, 2, chunks)),
                dma((3, 2, chunks)),
                dma((3, 2, chunks)),
                dma((3, 2, chunks)),
                dma((span,)),
                dma((slots,)),
                dma((2, span)),
                dma((2, slots)),
                dma((span,)),
                dma((slots,)),
                dma((2, span)),
                dma((2, slots)),
            ],
            compiler_params=pltpu.CompilerParams(
                collective_id=0, has_side_effects=True, vmem_limit_bytes=48 * 1024 * 1024
            ),
        )(*[
            pltpu.with_memory_space_constraint(z, pltpu.HBM)
            for z in (east, north, salt, surface, depth, wet, active)
        ])
        return pl.pallas_call(
            finish,
            out_shape=(state, state, state, jax.ShapeDtypeStruct(surface.shape, f32)),
            in_specs=[block] * 5,
            out_specs=(hbm,) * 4,
            scratch_shapes=[vmem((2,) + east.shape, f32), dma((4,))],
            compiler_params=pltpu.CompilerParams(vmem_limit_bytes=8 * 1024 * 1024),
        )(state3, slopes, surface_next, wet, active)

    return jax.shard_map(
        local,
        mesh=mesh,
        in_specs=(
            P(None, "gx", "gy"),
            P(None, "gx", "gy"),
            P(None, "gx", "gy"),
            P("gx", "gy"),
            P("gx", "gy"),
            P("gx", "gy"),
            P("gx", "gy"),
        ),
        out_specs=(P(None, "gx", "gy"), P(None, "gx", "gy"), P(None, "gx", "gy"), P("gx", "gy")),
        check_vma=False,
    )
```
